32 devices in a mesh: dp: 16 (over z, y, core), tensor: 2 (over x).
Axes of the slice: x: 2, y: 2, z: 4, core: 2. Of those that a mesh axis runs over, the one named last changes fastest.
Arguments:
- noisy_sample: float32 [2048, 28], P('dp'), may hold values from -5 to 5
- timestep: int32 [2048], P('dp'), may hold values from 0 to 99
- noise: float32 [2048, 28], P('dp'), may hold values from -5 to 5
- obs_feat: bfloat16 [2048, 1024], P('dp'), may hold values from -6 to 6
- step_w1: bfloat16 [256, 1024], replicated, may hold values from -0.75 to 0.75
- step_w2: bfloat16 [1024, 256], replicated, may hold values from -0.25 to 0.25
- film_weight: bfloat16 [1280, 2, 4096], P('dp', None, 'tensor'), may hold values from -0.25 to 0.25
- conv_in_w: bfloat16 [5, 7, 4096], P(None, None, 'tensor'), may hold values from -1 to 1
- residual_w: bfloat16 [7, 4096], P(None, 'tensor'), may hold values from -2 to 2
- conv_mid_w: bfloat16 [5, 4096, 4096], P(None, 'dp', 'tensor'), may hold values from -0.0390625 to 0.0390625
- out_w: bfloat16 [4096, 7], P('tensor'), may hold values from -0.1875 to 0.1875
- gain_one: float32 [4096], P('tensor'), may hold values from 0.4 to 1.6
- gain_two: float32 [4096], P('tensor'), may hold values from 0.4 to 1.6
Outputs:
- predicted_noise: float32 [2048, 28], P('dp')
- denoised: float32 [2048, 28], P('dp')
The draws below stay inside these ranges and needn't reach their ends.
All inputs are finite; a program needn't handle non-finite values.
Results may differ from the reference program's by a relative error of at most 0.0046.
Values may be sent and summed in bfloat16 or wider, within the bound.
A program may use at most 192 MiB of HBM per device.

```python
import math
import jax
import jax.numpy as jnp
from jax import lax

C = 4096
ACT = 7
HORIZON = 4
TAPS = 5
GROUPS = 8
STEP = 256
STEP_HID = 1024
OBS_FEAT = 1024
TRAIN_STEPS = 100
COND = 1280
OBS = 2048


def set_ends(result, rng, smallest, largest):
    longest = result.shape.index(max(result.shape))
    spots = []
    for shift in (0, 1):
        where = [jax.random.randint(jax.random.fold_in(rng, axis), (), 0, length) for axis, length in enumerate(result.shape)]
        where[longest] = (where[longest] + shift) % result.shape[longest]
        spots.append(tuple(where))
    return result.at[spots[0]].set(smallest).at[spots[1]].set(largest)


def levels(key, shape, shards, smallest, largest):
    loudness, own = 1.0, jax.random.fold_in(key, 6)
    for axis_at, blocks in shards:
        heights = jnp.exp(jax.random.uniform(jax.random.fold_in(own, axis_at), (blocks,), jnp.float32, smallest / len(shards), largest / len(shards)))
        loudness = loudness * jnp.repeat(heights, shape[axis_at] // blocks).reshape([-1 if axis == axis_at else 1 for axis in range(len(shape))])
    return loudness


def scatter_about(own_key, dims, scale, bound, cuts=(), kind=jnp.bfloat16):
    values = scale * jax.random.normal(own_key, dims, jnp.float32)
    if cuts:
        values = values * levels(own_key, dims, cuts, -0.22, 0.18)
    return jnp.clip(values, -bound, bound).astype(kind)


def setup_inputs(seed: int = 0) -> dict:
    streams_of = jax.random.split(jax.random.key(seed), 14)
    noisy_sample = scatter_about(streams_of[0], (OBS, HORIZON * ACT), 1.0, 5.0, ((0, 16),), jnp.float32)
    timestep = set_ends(jax.random.randint(streams_of[1], (OBS,), 0, TRAIN_STEPS), jax.random.fold_in(streams_of[1], 1), 0, TRAIN_STEPS - 1).astype(jnp.int32)
    noise = scatter_about(streams_of[2], (OBS, HORIZON * ACT), 1.0, 5.0, ((0, 16),), jnp.float32)
    obs_feat = scatter_about(streams_of[3], (OBS, OBS_FEAT), 1.0, 6.0, ((0, 16),))
    step_w1 = scatter_about(streams_of[4], (STEP, STEP_HID), (STEP // 4) ** -0.5, 0.75)
    step_w2 = scatter_about(streams_of[5], (STEP_HID, STEP), (STEP_HID // 2) ** -0.5, 0.25)
    film_weight = scatter_about(streams_of[6], (COND, 2, C), (COND // 2) ** -0.5, 0.25, ((0, 16), (2, 2)))
    conv_in_w = scatter_about(streams_of[7], (TAPS, ACT, C), (TAPS * ACT) ** -0.5, 1.0, ((2, 2),))
    residual_w = scatter_about(streams_of[8], (ACT, C), ACT ** -0.5, 2.0, ((1, 2),))
    conv_mid_w = scatter_about(streams_of[9], (TAPS, C, C), (TAPS * C) ** -0.5, 0.0390625, ((1, 16), (2, 2)))
    out_w = scatter_about(streams_of[10], (C, ACT), (C // 4) ** -0.5, 0.1875, ((0, 2),))
    gain_one = jnp.clip(0.4 + 1.2 * jax.random.uniform(streams_of[11], (C,), jnp.float32) ** levels(streams_of[11], (C,), ((0, 2),), -0.2, 0.2), 0.4, 1.6)
    gain_two = jnp.clip(0.4 + 1.2 * jax.random.uniform(streams_of[12], (C,), jnp.float32) ** levels(streams_of[12], (C,), ((0, 2),), -0.2, 0.2), 0.4, 1.6)
    return dict(noisy_sample=noisy_sample, timestep=timestep, noise=noise, obs_feat=obs_feat, step_w1=step_w1, step_w2=step_w2, film_weight=film_weight, conv_in_w=conv_in_w, residual_w=residual_w, conv_mid_w=conv_mid_w, out_w=out_w, gain_one=gain_one, gain_two=gain_two)


def plan():
    pos = jnp.arange(TRAIN_STEPS + 1, dtype=jnp.float32) / TRAIN_STEPS
    curve = jnp.cos((pos + 0.008) / 1.008 * (math.pi / 2)) ** 2
    betas = jnp.minimum(1.0 - curve[1:] / curve[:-1], 0.999)
    return jnp.cumprod(1.0 - betas)

def lookup(table, steps):
    onehot = (steps[:, None] == jnp.arange(table.shape[0], dtype=jnp.int32)[None, :]).astype(jnp.float32)
    return lax.optimization_barrier(jnp.sum(onehot * table[None, :], axis=1))

def mish(value):
    return value * jnp.tanh(jax.nn.softplus(value))

def sinusoid(steps):
    half = STEP // 2
    freqs = jnp.exp(jnp.arange(half, dtype=jnp.float32) * (-math.log(10000.0) / (half - 1)))
    angles = steps.astype(jnp.float32)[:, None] * freqs[None, :]
    return jnp.concatenate([jnp.sin(angles), jnp.cos(angles)], axis=1)

def convolve(acts, weight):
    count, length, inner = acts.shape
    padded = jnp.pad(acts, ((0, 0), (2, 2), (0, 0)))
    total = jnp.zeros((count * length, weight.shape[2]), jnp.float32)
    for shift in range(TAPS):
        window = padded[:, shift:shift + length, :].reshape(count * length, inner)
        total = total + jnp.dot(window, weight[shift], preferred_element_type=jnp.float32)
    return total.reshape(count, length, weight.shape[2])

def group_norm(hidden, gain, groups):
    count, length, width = hidden.shape
    split = hidden.reshape(count, length, groups, width // groups)
    mean = lax.optimization_barrier(jnp.mean(split, axis=(1, 3), keepdims=True))
    var = lax.optimization_barrier(jnp.mean((split - mean) ** 2, axis=(1, 3), keepdims=True))
    normed = ((split - mean) / jnp.sqrt(var + 1e-05)).reshape(count, length, width)
    return normed * gain[None, None, :]

def denoise_step(sample, eps, noise, steps):
    alpha_bar = plan()
    now = lookup(alpha_bar, steps)[:, None]
    before = jnp.where(steps > 0, lookup(alpha_bar, jnp.maximum(steps - 1, 0)), 1.0)[:, None]
    beta_prod = 1.0 - now
    cur_alpha = now / before
    cur_beta = 1.0 - cur_alpha
    start = jnp.clip((sample - jnp.sqrt(beta_prod) * eps) / jnp.sqrt(now), -1.0, 1.0)
    mean = jnp.sqrt(before) * cur_beta / beta_prod * start + jnp.sqrt(cur_alpha) * (1.0 - before) / beta_prod * sample
    spread = jnp.sqrt((1.0 - before) / beta_prod * cur_beta)
    return mean + spread * noise

def reference(noisy_sample, timestep, noise, obs_feat, step_w1, step_w2, film_weight, conv_in_w, residual_w, conv_mid_w, out_w, gain_one, gain_two):
    count = noisy_sample.shape[0]
    sample_b = noisy_sample.reshape(count, HORIZON, ACT).astype(jnp.bfloat16)
    sinus = sinusoid(timestep).astype(jnp.bfloat16)
    step_hidden = mish(jnp.dot(sinus, step_w1, preferred_element_type=jnp.float32)).astype(jnp.bfloat16)
    step_feat = jnp.dot(step_hidden, step_w2, preferred_element_type=jnp.float32)
    cond = mish(jnp.concatenate([step_feat, obs_feat.astype(jnp.float32)], axis=1)).astype(jnp.bfloat16)
    film = jnp.dot(cond, film_weight.reshape(COND, 2 * C), preferred_element_type=jnp.float32)
    scale = film[:, :C]
    shift = film[:, C:]
    first = mish(group_norm(convolve(sample_b, conv_in_w), gain_one, GROUPS))
    act_one = (scale[:, None, :] * first + shift[:, None, :]).astype(jnp.bfloat16)
    skip = jnp.dot(sample_b.reshape(count * HORIZON, ACT), residual_w, preferred_element_type=jnp.float32).reshape(count, HORIZON, C)
    act_two = (mish(group_norm(convolve(act_one, conv_mid_w), gain_two, GROUPS)) + skip).astype(jnp.bfloat16)
    eps = jnp.dot(act_two.reshape(count * HORIZON, C), out_w, preferred_element_type=jnp.float32).reshape(count, HORIZON * ACT)
    denoised = denoise_step(noisy_sample, eps, noise, timestep)
    return (eps, denoised)
```

```python
import math

import jax
import jax.numpy as jnp
from jax import lax
from jax.experimental import pallas as pl
from jax.experimental.pallas import tpu as pltpu
from jax.sharding import Mesh
from jax.sharding import PartitionSpec as P

C = 4096
ACT = 7
HORIZON = 4
TAPS = 5
GROUPS = 8
STEP = 256
TRAIN_STEPS = 100


def plan():
    pos = jnp.arange(TRAIN_STEPS + 1, dtype=jnp.float32) / TRAIN_STEPS
    curve = jnp.cos((pos + 0.008) / 1.008 * (math.pi / 2)) ** 2
    betas = jnp.minimum(1.0 - curve[1:] / curve[:-1], 0.999)
    return jnp.cumprod(1.0 - betas)


def lookup(table, steps):
    onehot = (steps[:, None] == jnp.arange(table.shape[0], dtype=jnp.int32)[None, :]).astype(
        jnp.float32
    )
    return jnp.sum(onehot * table[None, :], axis=1)


def mish(value):
    e = jnp.exp(jnp.minimum(value, 20.0))
    n = e * (e + 2.0)
    return value * (n / (n + 2.0))


def sinusoid(steps):
    half = STEP // 2
    freqs = jnp.exp(jnp.arange(half, dtype=jnp.float32) * (-math.log(10000.0) / (half - 1)))
    angles = steps.astype(jnp.float32)[:, None] * freqs[None, :]
    return jnp.concatenate([jnp.sin(angles), jnp.cos(angles)], axis=1)


def denoise_step(sample, eps, noise, steps):
    alpha_bar = plan()
    now = lookup(alpha_bar, steps)[:, None]
    before = jnp.where(steps > 0, lookup(alpha_bar, jnp.maximum(steps - 1, 0)), 1.0)[:, None]
    beta_prod = 1.0 - now
    cur_alpha = now / before
    cur_beta = 1.0 - cur_alpha
    start = jnp.clip((sample - jnp.sqrt(beta_prod) * eps) / jnp.sqrt(now), -1.0, 1.0)
    mean = (
        jnp.sqrt(before) * cur_beta / beta_prod * start
        + jnp.sqrt(cur_alpha) * (1.0 - before) / beta_prod * sample
    )
    spread = jnp.sqrt((1.0 - before) / beta_prod * cur_beta)
    return mean + spread * noise


DEPTH_PARTS = 4
PARTS = 2
VMEM = 60 * 1024 * 1024


def first_kernel(blocks, x_ref, wt_ref, cond_ref, film_ref, gain_ref, out_ref):
    x = x_ref[...]
    hs = [
        jnp.dot(x, wt_ref[h], preferred_element_type=jnp.float32) for h in range(HORIZON)
    ]
    width = hs[0].shape[1]
    count = HORIZON * width
    mean = sum(jnp.sum(h, axis=1, keepdims=True) for h in hs) / count
    hs = [h - mean for h in hs]
    var = sum(jnp.sum(h * h, axis=1, keepdims=True) for h in hs) / count
    inv = 1.0 / jnp.sqrt(var + 1e-05)
    cond = cond_ref[...]
    scale = jnp.dot(cond, film_ref[0], preferred_element_type=jnp.float32)
    shift = jnp.dot(cond, film_ref[1], preferred_element_type=jnp.float32)
    gain = gain_ref[...]
    cl = width // blocks
    for h in range(HORIZON):
        val = (scale * mish(hs[h] * inv * gain) + shift).astype(jnp.bfloat16)
        for b in range(blocks):
            out_ref[b, :, h * cl : (h + 1) * cl] = val[:, b * cl : (b + 1) * cl]


def first_stage(xs, wt, cond, film, gain, blocks, cl):
    rows = xs.shape[0]
    width = wt.shape[2]
    gw = C // GROUPS
    per = gw // cl
    rt = min(128, rows)
    inner = cond.shape[1]
    kern = lambda *refs: first_kernel(per, *refs)
    return pl.pallas_call(
        kern,
        grid=(width // gw, rows // rt),
        in_specs=[
            pl.BlockSpec((rt, xs.shape[1]), lambda g, r: (r, 0)),
            pl.BlockSpec((HORIZON, wt.shape[1], gw), lambda g, r: (0, 0, g)),
            pl.BlockSpec((rt, inner), lambda g, r: (r, 0)),
            pl.BlockSpec((2, inner, gw), lambda g, r: (0, 0, g)),
            pl.BlockSpec((1, gw), lambda g, r: (0, g)),
        ],
        out_specs=pl.BlockSpec((per, rt, HORIZON * cl), lambda g, r: (g, r, 0)),
        out_shape=jax.ShapeDtypeStruct((blocks, rows, HORIZON * cl), jnp.bfloat16),
        compiler_params=pltpu.CompilerParams(vmem_limit_bytes=VMEM),
        cost_estimate=pl.CostEstimate(
            flops=4 * rows * inner * width,
            bytes_accessed=4 * inner * width + 2 * rows * width * HORIZON,
            transcendentals=rows * width * HORIZON,
        ),
        name="first_stage",
    )(xs, wt, cond, film, gain)


def mix_kernel(pieces, mid, order_ref, *refs):
    a_ref, w_refs, out_ref = refs[0], refs[1 : 1 + pieces], refs[1 + pieces]
    cl = w_refs[0].shape[0] // TAPS
    parts, _, rows, _ = out_ref.shape
    for h in range(HORIZON):
        p0 = max(0, h - mid)
        p1 = min(HORIZON, h - mid + TAPS)
        k0 = p0 - h + mid
        k1 = p1 - h + mid
        acc = None
        for i in range(pieces):
            left = a_ref[order_ref[i], :, p0 * cl : p1 * cl]
            term = jnp.dot(
                left, w_refs[i][k0 * cl : k1 * cl, :], preferred_element_type=jnp.float32
            )
            acc = term if acc is None else acc + term
        for q in range(parts):
            out_ref[q, h] = acc[q * rows : (q + 1) * rows].astype(jnp.bfloat16)


def mix(order, acts, pieces):
    n = len(pieces)
    rows = acts.shape[1]
    width = pieces[0].shape[1]
    nt = min(256, width)
    kern = lambda *refs: mix_kernel(n, TAPS // 2, *refs)
    return pl.pallas_call(
        kern,
        grid=(width // nt,),
        in_specs=[
            pl.BlockSpec(memory_space=pltpu.SMEM),
            pl.BlockSpec(acts.shape, lambda j: (0, 0, 0)),
        ]
        + [pl.BlockSpec((p.shape[0], nt), lambda j: (0, j)) for p in pieces],
        out_specs=pl.BlockSpec(
            (DEPTH_PARTS, HORIZON, rows // DEPTH_PARTS, nt), lambda j: (0, 0, 0, j)
        ),
        out_shape=jax.ShapeDtypeStruct(
            (DEPTH_PARTS, HORIZON, rows // DEPTH_PARTS, width), jnp.bfloat16
        ),
        compiler_params=pltpu.CompilerParams(vmem_limit_bytes=VMEM),
        cost_estimate=pl.CostEstimate(
            flops=2 * 14 * rows * n * pieces[0].shape[0] // TAPS * width,
            bytes_accessed=2 * n * pieces[0].shape[0] * width + 8 * rows * width,
            transcendentals=0,
        ),
        name="mix",
    )(order, acts, *pieces)


def hop(value, axis, step):
    size = lax.axis_size(axis)
    return lax.ppermute(value, axis, [(i, (i + step) % size) for i in range(size)])


def relative(value):
    return jnp.concatenate(
        [value] + [hop(value, "z", -q) for q in range(1, DEPTH_PARTS)], axis=0
    )


def reduce_parts(part):
    half = HORIZON // 2
    far = part[2]
    up = hop(far[:half], "z", 1)
    down = hop(far[half:], "z", -1)
    f32 = jnp.float32
    near_up = (part[1, :half].astype(f32) + up.astype(f32)).astype(jnp.bfloat16)
    near_down = (part[3, half:].astype(f32) + down.astype(f32)).astype(jnp.bfloat16)
    got = [
        (hop(near_up, "z", 1), hop(part[3, :half], "z", -1)),
        (hop(part[1, half:], "z", 1), hop(near_down, "z", -1)),
    ]
    out = []
    for h in range(HORIZON):
        one, two = got[h // half]
        out.append(
            part[0, h].astype(f32) + one[h % half].astype(f32) + two[h % half].astype(f32)
        )
    return out


def body(
    noisy_sample,
    timestep,
    noise,
    obs_feat,
    step_w1,
    step_w2,
    film_weight,
    conv_in_w,
    residual_w,
    conv_mid_w,
    out_w,
    gain_one,
    gain_two,
):
    count = noisy_sample.shape[0]
    local_width = conv_in_w.shape[2]
    cl = conv_mid_w.shape[1]
    yn = lax.axis_size("y")
    zi, yi, ci = lax.axis_index("z"), lax.axis_index("y"), lax.axis_index("c")
    blocks = yn * 2
    kw = cl * blocks
    step = local_width // PARTS
    pieces = []
    for n in range(PARTS):
        own = conv_mid_w.reshape(TAPS * cl, local_width)[:, n * step : (n + 1) * step]
        near = [own] + [hop(own, "y", -s) for s in range(1, yn)]
        pieces.append(near + [hop(v, "c", 1) for v in near])
    order = jnp.stack(
        [((yi + s) % yn) * 2 + ci for s in range(yn)]
        + [((yi + s) % yn) * 2 + (1 - ci) for s in range(yn)]
    ).astype(jnp.int32)
    film = jnp.transpose(film_weight, (1, 0, 2))
    film = lax.all_gather(film, "tensor", axis=2, tiled=True)
    film = lax.all_to_all(film, "z", split_axis=2, concat_axis=1, tiled=True)
    film = lax.all_gather(film, ("y", "c"), axis=1, tiled=True)
    win = lax.all_gather(conv_in_w, "tensor", axis=2, tiled=True)
    win = lax.dynamic_slice_in_dim(win, zi * kw, kw, 2)
    gain = lax.all_gather(gain_one, "tensor", axis=0, tiled=True)
    gain = lax.dynamic_slice_in_dim(gain, zi * kw, kw, 0)[None, :]
    toep = []
    for h in range(HORIZON):
        rows = []
        for p in range(HORIZON):
            k = p - h + TAPS // 2
            rows.append(win[k] if 0 <= k < TAPS else jnp.zeros((ACT, kw), win.dtype))
        toep.append(jnp.concatenate(rows, axis=0))
    toep = jnp.stack(toep)
    sample_b = noisy_sample.astype(jnp.bfloat16)
    sinus = sinusoid(timestep).astype(jnp.bfloat16)
    step_hidden = mish(jnp.dot(sinus, step_w1, preferred_element_type=jnp.float32)).astype(
        jnp.bfloat16
    )
    step_feat = jnp.dot(step_hidden, step_w2, preferred_element_type=jnp.float32)
    cond = mish(jnp.concatenate([step_feat, obs_feat.astype(jnp.float32)], axis=1)).astype(
        jnp.bfloat16
    )
    fr = film_weight.shape[0]
    cond = (
        cond.reshape(count, DEPTH_PARTS, blocks, fr)
        .transpose(0, 2, 1, 3)
        .reshape(count, cond.shape[1])
    )
    acts = first_stage(relative(sample_b), toep, relative(cond), film, gain, blocks, cl)
    found = [reduce_parts(mix(order, acts, p)) for p in pieces]
    hs = [jnp.concatenate([f[h] for f in found], axis=1) for h in range(HORIZON)]
    gw = C // GROUPS
    outs = []
    cols = [slice(g * gw, (g + 1) * gw) for g in range(local_width // gw)]
    stats = []
    for col in cols:
        mean = sum(jnp.sum(h[:, col], axis=1, keepdims=True) for h in hs) / (HORIZON * gw)
        var = sum(jnp.sum((h[:, col] - mean) ** 2, axis=1, keepdims=True) for h in hs) / (
            HORIZON * gw
        )
        stats.append((mean, 1.0 / jnp.sqrt(var + 1e-05)))
    mean = jnp.concatenate([jnp.broadcast_to(m, (count, gw)) for m, _ in stats], axis=1)
    inv = jnp.concatenate([jnp.broadcast_to(v, (count, gw)) for _, v in stats], axis=1)
    for h in range(HORIZON):
        skip = jnp.dot(
            sample_b[:, h * ACT : (h + 1) * ACT], residual_w, preferred_element_type=jnp.float32
        )
        normed = (hs[h] - mean) * inv * gain_two[None, :]
        act_two = (mish(normed) + skip).astype(jnp.bfloat16)
        outs.append(jnp.dot(act_two, out_w, preferred_element_type=jnp.float32))
    eps = lax.psum(jnp.concatenate(outs, axis=1), "tensor")
    denoised = denoise_step(noisy_sample, eps, noise, timestep)
    return (eps, denoised)


def solution(mesh):
    dp, tensor = mesh.shape["dp"], mesh.shape["tensor"]
    grid = Mesh(
        mesh.devices.reshape(DEPTH_PARTS, dp // DEPTH_PARTS // 2, 2, tensor),
        ("z", "y", "c", "tensor"),
    )
    rows = ("z", "y", "c")
    return jax.shard_map(
        body,
        mesh=grid,
        in_specs=(
            P(rows, None),
            P(rows),
            P(rows, None),
            P(rows, None),
            P(),
            P(),
            P(rows, None, "tensor"),
            P(None, None, "tensor"),
            P(None, "tensor"),
            P(None, rows, "tensor"),
            P("tensor", None),
            P("tensor"),
            P("tensor"),
        ),
        out_specs=(P(rows, None), P(rows, None)),
        check_vma=False,
    )
```
